32 devices in a mesh: grp: 8 (over z, x), slc: 4 (over y, core).
Axes of the slice: x: 2, y: 2, z: 4, core: 2. Of those that a mesh axis runs over, the one named last changes fastest.
Arguments:
- orbitals: float32 [64, 48, 2304], P('grp', 'slc'), may hold values from -6 to 6
- local_pot: float32 [64, 48, 2304], P('grp', 'slc'), may hold values from -1 to 1
- pair_owner: int32 [8, 8, 1], P('grp'), may hold values from 0 to 7; in each aligned block of 8 rows (0 to 7, 8 to 15, ..., all dimensions but the last counted through in order) at most 2 rows name the same one
- pair_remote: int32 [8, 8], P('grp'), may hold values from 0 to 7
- pair_resident: int32 [8, 8], P('grp'), may hold values from 0 to 1
- pair_count: int32 [8, 4], P('grp'), may hold values from 1 to 3, 8 in all within a row
- offsets: int32 [64, 3], replicated, may hold values from 0 to 23
Outputs:
- applied: float32 [64, 48, 2304], P('grp', 'slc')
The draws below stay inside these ranges and needn't reach their ends.
Inputs may be any that keep to these rules, and one draw needn't show every extreme that they name: `pair_owner`: within one group's 8 pairs no owner group is named more than 2 times, and some owner group is named exactly 2 times. `pair_count`: the 4 counts of one group sum to 8, and in every group some device has exactly 3.
All inputs are finite; a program needn't handle non-finite values.
Results may differ from the reference program's by a relative error of at most 0.0003.
Values sent between devices are 32-bit elements; how exact they have to be, the bound alone decides.
No kernel may reach another device: no remote copies, remote signals or barrier semaphores. Data moves between devices by JAX's collectives and lax.ppermute only.
A program may use at most 128 MiB of HBM per device.

```python
import math
import jax
import jax.numpy as jnp
import numpy as np
from jax import lax

B = 48
ORB_DEV = 2
PAIRS = 3
LIVE_GRP = 8
CAP = 2
SPREAD = 24
ORB_GRP = 8
ORBITALS = 64
N_GRP = 8
N_SLC = 4


def touch_ends(values, rng, least, top_value):
    index_at = [jax.random.randint(jax.random.fold_in(rng, axis), (), 0, length) for axis, length in enumerate(values.shape)]
    widest = values.shape.index(max(values.shape))
    beside = index_at[:widest] + [(index_at[widest] + 1) % values.shape[widest]] + index_at[widest + 1:]
    return values.at[tuple(index_at)].set(least).at[tuple(beside)].set(top_value)


def shard_levels(rng, shape, pieces, least, top_value):
    factor_of, own = 1.0, jax.random.fold_in(rng, 6)
    for dim, blocks in pieces:
        draws = jnp.exp(jax.random.uniform(jax.random.fold_in(own, dim), (blocks,), jnp.float32, least / len(pieces), top_value / len(pieces)))
        factor_of = factor_of * jnp.repeat(draws, shape[dim] // blocks).reshape([-1 if axis == dim else 1 for axis in range(len(shape))])
    return factor_of


def split_up(count, total, reach, lean):
    weights = [(1 << 20) // math.isqrt(standing ** lean) + 1 for standing in range(2, count + 1)]
    rest, given = total - reach - (count - 1), [1] * (count - 1)
    while rest > 0:
        candidates = [i for i in range(count - 1) if given[i] < reach]
        mass, remaining = sum([weights[i] for i in candidates]), rest
        for i in candidates:
            more = min(reach - given[i], max(1, remaining * weights[i] // mass), rest)
            given[i] = given[i] + more
            rest = rest - more
    return np.array([reach] + given)


def ragged_sizes(key, number_of, total, reach, lean):
    if number_of == 2:
        one = jax.random.randint(key, (), max(1, total - reach), min(reach, total - 1) + 1)
        return jnp.stack([one, total - one])
    sizes = jnp.asarray(split_up(number_of, total, reach, lean), jnp.int32)
    pairs = (number_of - 1) // 2
    giver, sink = sizes[1:1 + 2 * pairs:2], sizes[2:2 + 2 * pairs:2]
    slack = jnp.minimum(giver - 1, reach - sink)
    moved = jax.random.randint(jax.random.fold_in(key, 1), (pairs,), 0, 1 << 20) % (slack + 1)
    sizes = sizes.at[1:1 + 2 * pairs:2].set(giver - moved).at[2:2 + 2 * pairs:2].set(sink + moved)
    return sizes[jax.random.permutation(jax.random.fold_in(key, 2), number_of)]


def deal_out(rng, own, number, rows, count, top, bound, skew):
    sequence = jax.random.permutation(rng, count)
    crowded, common = portions_of(count, rows * top, bound, skew, True), portions_of(count, rows * top, bound, skew, False)
    places = jnp.arange(count)

    def named(sizes, turn):
        used = int((sizes > 0).sum())
        fixed = max(1, used // 4)
        moved = fixed + (places - fixed + turn * (used - fixed)) % max(1, count - fixed)
        return jnp.zeros((count,), jnp.int32).at[sequence[jnp.where(places < fixed, places, moved)]].set(jnp.asarray(sizes, jnp.int32))

    sizes = jnp.where(number % 4 == 0, named(crowded, number // 4), named(common, number - number // 4 - 1))
    mixed = jax.random.permutation(jax.random.fold_in(own, 3), count)
    source_of, taker = mixed[0:count // 2 * 2:2], mixed[1:count // 2 * 2:2]
    room = jnp.minimum(sizes[source_of] - 1, bound - sizes[taker]) // 2
    room = jnp.where((source_of == sequence[0]) | (taker == sequence[0]) | (sizes[taker] == 0), 0, jnp.maximum(room, 0))
    moved = jax.random.randint(jax.random.fold_in(own, 4), (count // 2,), 0, 1 << 20) % (room + 1)
    sizes = sizes.at[source_of].add(-moved).at[taker].add(moved)
    items = jnp.searchsorted(jnp.cumsum(sizes), jnp.arange(rows * top), side="right").astype(jnp.int32)
    listing = items.reshape(top, rows).T
    listing = listing[jax.random.permutation(jax.random.fold_in(own, 1), rows)]
    turn = jax.random.randint(jax.random.fold_in(own, 2), (rows, 1), 0, top)
    return jnp.take_along_axis(listing, (jnp.arange(top)[None, :] + turn) % top, axis=1)


def portions_of(number_of, total, reach, lean, full):
    portions = [(1 << 20) // math.isqrt(standing ** lean) + 1 for standing in range(1, number_of + 1)]
    largest = reach if full else min(reach, max(-(-total // number_of), total * portions[0] // sum(portions)))
    least = 1 if total - largest >= number_of - 1 else 0
    holding, rest = [largest] + [least] * (number_of - 1), total - largest - least * (number_of - 1)
    while rest > 0:
        movable = [i for i in range(1, number_of) if holding[i] < largest] or [i for i in range(1, number_of) if holding[i] < reach]
        whole, left = sum([portions[i] for i in movable]), rest
        for i in movable:
            more = min(reach - holding[i], max(1, left * portions[i] // whole), rest)
            holding[i] = holding[i] + more
            rest = rest - more
    return np.array(holding)


def scatter_about(key, extent, scale, most, pieces=(), kind=jnp.bfloat16):
    level = shard_levels(key, extent, pieces, -0.22, 0.18) if pieces else 1.0
    values = jax.random.normal(key, extent, jnp.float32) * scale * level
    return jnp.minimum(jnp.maximum(values, -most), most).astype(kind)


def setup_inputs(seed: int = 0) -> dict:
    key_of = jax.random.split(jax.random.key(seed), 8)
    orbitals = scatter_about(key_of[0], (ORBITALS, B, B * B), 1.0, 6.0, ((0, 8), (1, 4)), jnp.float32)
    local_pot = jnp.clip(jax.random.uniform(key_of[1], (ORBITALS, B, B * B), jnp.float32, -1.0, 1.0) * shard_levels(key_of[1], (ORBITALS, B, B * B), ((0, 8), (1, 4)), -0.4, 0.0), -1.0, 1.0)
    pair_owner_keys = jax.random.split(jax.random.fold_in(key_of[2], 1), N_GRP * LIVE_GRP // LIVE_GRP)
    pair_owner_turns = jax.random.permutation(jax.random.fold_in(key_of[2], 3), N_GRP * LIVE_GRP // LIVE_GRP)
    pair_owner = jax.vmap(lambda own, number: deal_out(jax.random.fold_in(key_of[2], 2), own, number, LIVE_GRP, N_GRP, 1, CAP, 2))(pair_owner_keys, pair_owner_turns).reshape((N_GRP, LIVE_GRP, 1))
    pair_remote = touch_ends(jax.random.randint(key_of[3], (N_GRP, LIVE_GRP), 0, ORB_GRP), jax.random.fold_in(key_of[3], 1), 0, ORB_GRP - 1).astype(jnp.int32)
    pair_resident = touch_ends(jax.random.randint(key_of[4], (N_GRP, LIVE_GRP), 0, ORB_DEV), jax.random.fold_in(key_of[4], 1), 0, ORB_DEV - 1).astype(jnp.int32)
    pair_count = jax.vmap(lambda own: ragged_sizes(own, N_SLC, LIVE_GRP, PAIRS, 2))(jax.random.split(key_of[5], N_GRP)).reshape((N_GRP, N_SLC)).astype(jnp.int32)
    offsets = touch_ends(jax.random.randint(key_of[6], (ORBITALS, 3), 0, SPREAD), jax.random.fold_in(key_of[6], 1), 0, SPREAD - 1).astype(jnp.int32)
    return {"orbitals": orbitals, "local_pot": local_pot, "pair_owner": pair_owner, "pair_remote": pair_remote, "pair_resident": pair_resident, "pair_count": pair_count, "offsets": offsets}


highest = lax.Precision.HIGHEST
coupling = 1.0

def sine_table(box_edge):
    positions = jnp.arange(box_edge, dtype=jnp.float32)
    phases = jnp.pi * (positions[:, None] + 1.0) * (positions[None, :] + 1.0) / (box_edge + 1.0)
    return jnp.sqrt(2.0 / (box_edge + 1.0)) * jnp.sin(phases)

def kernel_weights(box_edge):
    positions = jnp.arange(box_edge, dtype=jnp.float32)
    eigenvalues = 2.0 - 2.0 * jnp.cos(jnp.pi * (positions + 1.0) / (box_edge + 1.0))
    return coupling / (eigenvalues[:, None, None] + eigenvalues[None, :, None] + eigenvalues[None, None, :])

def shift_matrix(amount, box_edge):
    positions = jnp.arange(box_edge, dtype=jnp.int32)
    return (positions[None, :] == positions[:, None] + amount).astype(jnp.float32)

def three_ways(mat_first, mat_second, mat_third, box_values):
    box_values = jnp.einsum('ka,abc->bck', mat_first, box_values, precision=highest)
    box_values = jnp.einsum('ka,abc->bck', mat_second, box_values, precision=highest)
    return jnp.einsum('ka,abc->bck', mat_third, box_values, precision=highest)

def one_pair(resident_box, partner_box, offset_gap, sine_rows, weights):
    box_edge = resident_box.shape[0]
    shift_first = shift_matrix(offset_gap[0], box_edge)
    shift_second = shift_matrix(offset_gap[1], box_edge)
    shift_third = shift_matrix(offset_gap[2], box_edge)
    shifted = three_ways(shift_first, shift_second, shift_third, partner_box)
    density = resident_box * shifted
    spectrum = three_ways(sine_rows, sine_rows, sine_rows, density)
    potential = three_ways(sine_rows, sine_rows, sine_rows, weights * spectrum)
    near_field = potential * shifted
    far_field = three_ways(shift_first.T, shift_second.T, shift_third.T, potential * resident_box)
    return (near_field, far_field)

def reference(orbitals, local_pot, pair_owner, pair_remote, pair_resident, pair_count, offsets):
    orbital_boxes = orbitals.reshape(ORBITALS, B, B, B)
    place = jnp.arange(LIVE_GRP, dtype=jnp.int32)
    running = jnp.cumsum(pair_count.astype(jnp.int32), axis=1)
    device_of = lax.optimization_barrier(jnp.sum((running[:, None, :] <= place[None, :, None]).astype(jnp.int32), axis=2))
    group_of = jnp.arange(N_GRP, dtype=jnp.int32)[:, None] + jnp.zeros((1, LIVE_GRP), jnp.int32)
    resident = (group_of * ORB_GRP + device_of * ORB_DEV + pair_resident.astype(jnp.int32)).reshape(-1)
    partner = (pair_owner[:, :, 0].astype(jnp.int32) * ORB_GRP + pair_remote.astype(jnp.int32)).reshape(-1)
    offset_gaps = jnp.take(offsets, resident, axis=0) - jnp.take(offsets, partner, axis=0)
    sine_rows = sine_table(B)
    weights = kernel_weights(B)

    def pair_step(fields, scan_item):
        near_index, far_index, offset_gap = scan_item
        near_field, far_field = one_pair(orbital_boxes[near_index], orbital_boxes[far_index], offset_gap, sine_rows, weights)
        fields = fields.at[near_index].add(near_field)
        fields = fields.at[far_index].add(far_field)
        return (fields, None)
    start = jnp.zeros((ORBITALS, B, B, B), jnp.float32)
    fields, unused = lax.scan(pair_step, start, (resident, partner, offset_gaps))
    return local_pot * orbitals - fields.reshape(orbitals.shape)
```

```python
import functools
import jax
import jax.numpy as jnp
import numpy as np
from jax import lax
from jax.experimental import pallas as pl
from jax.experimental.pallas import tpu as pltpu
from jax.sharding import PartitionSpec as P

B = 48
CAP = 2
LANES = 128
COLS = B * B // LANES
BLK = 3 * LANES
ROWS_BLK = BLK // B
NBLK = COLS // 3
PITCH = 56
PAD = (B // 2) * COLS
BOX = B * COLS


def sine_np():
    k = np.arange(B)
    return (np.sqrt(2.0 / (B + 1)) * np.sin(np.pi * (k[:, None] + 1) * (k[None, :] + 1) / (B + 1.0))).astype(
        np.float32
    )


def lam_np():
    k = np.arange(B)
    return 2.0 - 2.0 * np.cos(np.pi * (k + 1.0) / (B + 1.0))


def split(x):
    high = x.astype(jnp.bfloat16)
    return high, (x - high.astype(jnp.float32)).astype(jnp.bfloat16)


def mm(a, b):
    return jnp.dot(a, b, preferred_element_type=jnp.float32)


def mm3(ah, al, bh, bl):
    return mm(ah, bh) + mm(al, bh) + mm(ah, bl)


FWD_K = ((0, 128), (0, 256), (128, 384), (256, 384))


def tables_kernel(sine, wide, lams, sine3, fwd_h, fwd_l, inv_h, inv_l, weight):
    q = sine[...]
    qh, ql = split(q)
    q48h, q48l = qh[:, :B], ql[:, :B]
    sine3[...] = jnp.concatenate([q48h, q48h, q48l], axis=1)
    fwd_h[...] = jnp.zeros(fwd_h.shape, jnp.bfloat16)
    fwd_l[...] = jnp.zeros(fwd_l.shape, jnp.bfloat16)
    for b in range(ROWS_BLK):
        fwd_h[b * B : (b + 1) * B, b * LANES : (b + 1) * LANES] = qh
        fwd_l[b * B : (b + 1) * B, b * LANES : (b + 1) * LANES] = ql
    lane = lax.broadcasted_iota(jnp.int32, (LANES, BLK), 1)
    w = jnp.concatenate([wide[...], jnp.zeros((LANES - B, BLK), jnp.float32)], axis=0)
    for b in range(ROWS_BLK):
        part = jnp.where((lane >= b * B) & (lane < (b + 1) * B), w, 0.0)
        ph, plo = split(part)
        inv_h[b * LANES : (b + 1) * LANES, :] = ph
        inv_l[b * LANES : (b + 1) * LANES, :] = plo
    pair = lams[...]
    for k, lam in enumerate(lam_np()):
        weight[:, k * LANES : (k + 1) * LANES] = 1.0 / (pair + np.float32(lam))


def make_tables():
    q = sine_np()
    padded = np.zeros((B, LANES), np.float32)
    padded[:, :B] = q
    wide = np.tile(q, (1, ROWS_BLK))
    lam = lam_np()
    lam3 = np.ones((LANES,))
    lam3[:B] = lam
    lams = (lam[:, None] + lam3[None, :]).astype(np.float32)
    shapes = (
        jax.ShapeDtypeStruct((B, 3 * B), jnp.bfloat16),
        jax.ShapeDtypeStruct((BLK, ROWS_BLK * LANES), jnp.bfloat16),
        jax.ShapeDtypeStruct((BLK, ROWS_BLK * LANES), jnp.bfloat16),
        jax.ShapeDtypeStruct((ROWS_BLK * LANES, BLK), jnp.bfloat16),
        jax.ShapeDtypeStruct((ROWS_BLK * LANES, BLK), jnp.bfloat16),
        jax.ShapeDtypeStruct((B, B * LANES), jnp.float32),
    )
    return pl.pallas_call(tables_kernel, out_shape=shapes, name="tables")(
        jnp.asarray(padded), jnp.asarray(wide), jnp.asarray(lams)
    )


def one_slot(near, box, shifted, left_h, left_l, mid, mid2, inv_lh, inv_ll, sine3, fwd_h, fwd_l, inv_h, inv_l, weight, spots, out, e0, e1, e2):
    lane = lax.broadcasted_iota(jnp.int32, (B, LANES), 1)

    def turned(source, d0, d1, d2, j_list):
        flat = d0 * (B * B) + d1 * B + d2
        rows = lax.shift_right_arithmetic(flat, 7)
        rest = flat & (LANES - 1)
        back = (LANES - rest) & (LANES - 1)
        rolled = {}
        for j in j_list + [j_list[-1] + 1]:
            rolled[j] = pltpu.roll(source[pl.ds(PAD + rows + j, B, stride=COLS), :], back, axis=1)
        results = []
        for j in j_list:
            moved = jnp.where(lane < LANES - rest, rolled[j], rolled[j + 1])
            bb = spots[j : j + 1, :] + d1
            cc = spots[COLS + j : COLS + j + 1, :] + d2
            inside = (bb >= 0) & (bb < B) & (cc >= 0) & (cc < B)
            results.append(jnp.where(inside, moved, 0.0))
        return results

    s3 = sine3[...]

    def along_first(x):
        xh, xl = split(x)
        return mm(s3, jnp.concatenate([xh, xl, xh], axis=0))

    for m in range(NBLK):
        js = [3 * m, 3 * m + 1, 3 * m + 2]
        parts = turned(box, e0, e1, e2, js)
        dens = []
        for j, part in zip(js, parts):
            shifted[j * B : (j + 1) * B, :] = part
            dens.append(part * near[pl.ds(j, B, stride=COLS), :])
        yh, yl = split(along_first(jnp.concatenate(dens, axis=1)))
        left_h[m * B : (m + 1) * B, :] = yh
        left_l[m * B : (m + 1) * B, :] = yl
    for p, (lo, hi) in enumerate(FWD_K):
        cols = slice(p * 2 * LANES, (p + 1) * 2 * LANES)
        y = mm3(left_h[:, lo:hi], left_l[:, lo:hi], fwd_h[lo:hi, cols], fwd_l[lo:hi, cols])
        for m in range(NBLK):
            for h in range(2):
                b = ROWS_BLK * m + 2 * p + h
                mid[pl.ds(b, B, stride=PITCH), :] = y[m * B : (m + 1) * B, h * LANES : (h + 1) * LANES]
    group = 6

    def second(i, carry):
        first = i * group
        z = jnp.concatenate(
            [mid[pl.ds(pl.multiple_of((first + u) * PITCH, 8), B), :] for u in range(group)], axis=1
        )
        y = along_first(z) * weight[:, pl.ds(pl.multiple_of(first * LANES, LANES), group * LANES)]
        y = along_first(y)
        for u in range(group):
            mid2[pl.ds(first + u, B, stride=PITCH), :] = y[:, u * LANES : (u + 1) * LANES]
        return carry

    lax.fori_loop(0, B // group, second, 0)
    for m in range(NBLK):
        for b in range(ROWS_BLK):
            start = (ROWS_BLK * m + b) * PITCH
            zh, zl = split(mid2[start : start + B, :])
            inv_lh[m * B : (m + 1) * B, b * LANES : (b + 1) * LANES] = zh
            inv_ll[m * B : (m + 1) * B, b * LANES : (b + 1) * LANES] = zl
    ka = slice(0, 6 * LANES)
    kb = slice(5 * LANES, 8 * LANES)
    ya = mm3(inv_lh[:, ka], inv_ll[:, ka], inv_h[ka, : 2 * LANES], inv_l[ka, : 2 * LANES])
    yb = mm3(inv_lh[:, kb], inv_ll[:, kb], inv_h[kb, 2 * LANES :], inv_l[kb, 2 * LANES :])
    for m in range(NBLK):
        y = jnp.concatenate([ya[m * B : (m + 1) * B], yb[m * B : (m + 1) * B]], axis=1)
        pot = along_first(y)
        for u in range(3):
            j = 3 * m + u
            part = pot[:, u * LANES : (u + 1) * LANES]
            box[pl.ds(PAD + j, B, stride=COLS), :] = part * near[pl.ds(j, B, stride=COLS), :]
            out[0, pl.ds(j, B, stride=COLS), :] = part * shifted[j * B : (j + 1) * B, :]
    for m in range(NBLK):
        js = [3 * m, 3 * m + 1, 3 * m + 2]
        for j, part in zip(js, turned(box, -e0, -e1, -e2, js)):
            out[1, pl.ds(j, B, stride=COLS), :] = part


def pair_kernel(slices, slab, round_id, meta, tab, *refs):
    nears, refs = refs[:slices], refs[slices:]
    fars, refs = refs[:slices], refs[slices:]
    consts, refs = refs[:7], refs[7:]
    near_outs, refs = refs[:slices], refs[slices:]
    far_outs, refs = refs[:slices], refs[slices:]
    near, box, shifted, left_h, left_l, mid, mid2, inv_lh, inv_ll, out = refs
    own = meta[1]
    zeros = jnp.zeros((PAD, LANES), jnp.float32)
    box[:PAD, :] = zeros
    box[PAD + BOX :, :] = zeros
    for c in range(CAP):
        slot = (round_id * slices + own) * CAP + c

        @pl.when(tab[0, slot] > 0)
        def _():
            for k in range(slices):
                start = (own ^ k) * slab
                near[pl.ds(start, slab), :] = nears[k][c]
                box[pl.ds(PAD + start, slab), :] = fars[k][c]
            one_slot(near, box, shifted, left_h, left_l, mid, mid2, inv_lh, inv_ll, *consts, out, tab[2, slot], tab[3, slot], tab[4, slot])
            for k in range(slices):
                start = (own ^ k) * slab
                near_outs[k][c] = out[0, pl.ds(start, slab), :]
                far_outs[k][c] = out[1, pl.ds(start, slab), :]


def smem():
    return pl.BlockSpec(memory_space=pltpu.SMEM)


def vmem():
    return pl.BlockSpec(memory_space=pltpu.VMEM)


def pair_call(slices, slab, round_id, meta, tab, nears, fars, consts):
    spots = np.arange(B * B).reshape(COLS, LANES)
    spots = jnp.asarray(np.concatenate([spots // B, spots % B]).astype(np.int32))
    piece = (CAP, slab, LANES)
    shapes = [jax.ShapeDtypeStruct(piece, jnp.float32)] * (2 * slices)
    near_spec = pl.BlockSpec(piece, lambda i: (round_id, 0, 0))
    outs = pl.pallas_call(
        functools.partial(pair_kernel, slices, slab, round_id),
        grid=(1,),
        in_specs=[smem(), smem()] + [near_spec] * slices + [vmem()] * (slices + 7),
        out_specs=[vmem()] * (2 * slices),
        out_shape=shapes,
        scratch_shapes=[
            pltpu.VMEM((BOX, LANES), jnp.float32),
            pltpu.VMEM((BOX + 2 * PAD, LANES), jnp.float32),
            pltpu.VMEM((BOX, LANES), jnp.float32),
            pltpu.VMEM((NBLK * B, BLK), jnp.bfloat16),
            pltpu.VMEM((NBLK * B, BLK), jnp.bfloat16),
            pltpu.VMEM((B * PITCH, LANES), jnp.float32),
            pltpu.VMEM((B * PITCH, LANES), jnp.float32),
            pltpu.VMEM((NBLK * B, ROWS_BLK * LANES), jnp.bfloat16),
            pltpu.VMEM((NBLK * B, ROWS_BLK * LANES), jnp.bfloat16),
            pltpu.VMEM((2, BOX, LANES), jnp.float32),
        ],
        cost_estimate=pl.CostEstimate(flops=2 * 10**9, transcendentals=0, bytes_accessed=8 * 10**6),
        name="pairs",
    )(meta, tab, *nears, *fars, *consts, spots)
    return outs[:slices], outs[slices:]


def slab_pieces(orbs, planes, o):
    if orbs == 8:
        return [(o, planes * COLS, 0)]
    tiles = orbs // 8
    high = lax.shift_right_logical(o, 3)
    return [((a * tiles + high) * COLS * 8 + (o & 7), COLS, a * COLS) for a in range(planes)]


def near_kernel(groups, slices, listed, orbs, planes, meta, values, *refs):
    outs, (tab, seen) = refs[:slices], refs[slices:]
    gid = meta[0]
    own = meta[1]
    owner_at, remote_at, resident_at, count_at = 2, 2 + listed, 2 + 2 * listed, 2 + 3 * listed
    offset_at = count_at + slices
    for g in range(groups):
        seen[g] = 0
    for n in range(groups * CAP):
        tab[0, n] = 0

    def place(t, carry):
        running = 0
        home = 0
        for u in range(slices):
            running = running + meta[count_at + u]
            home = home + jnp.where(running <= t, 1, 0)
        owner = meta[owner_at + t]
        rank = seen[owner]
        seen[owner] = rank + 1
        n = (gid ^ owner) * CAP + rank
        local = home * (orbs // slices) + meta[resident_at + t]
        near_at = offset_at + 3 * (gid * orbs + local)
        far_at = offset_at + 3 * (owner * orbs + meta[remote_at + t])
        tab[0, n] = 1
        tab[1, n] = local
        for d in range(3):
            tab[2 + d, n] = meta[near_at + d] - meta[far_at + d]
        return carry

    lax.fori_loop(0, listed, place, 0)
    for k in range(slices):
        for q in range(groups // slices):
            for c in range(CAP):
                n = (q * slices + (own ^ k)) * CAP + c

                @pl.when(tab[0, n] > 0)
                def _():
                    for start, count, to in slab_pieces(orbs, planes, tab[1, n]):
                        outs[k][q * CAP + c, to : to + count, :] = values[pl.ds(start, count, stride=8), :]


def far_kernel(groups, slices, listed, orbs, planes, meta, lists, values, *refs):
    rounds = groups // slices
    outs, (tab,) = refs[: rounds * slices], refs[rounds * slices :]
    gid = meta[0]
    own = meta[1]
    for n in range(groups * CAP):
        tab[0, n] = 0

    def place(r, carry):
        def look(t, rank):
            hit = lists[gid ^ r, t] == gid

            @pl.when(hit)
            def _():
                tab[0, r * CAP + rank] = 1
                tab[1, r * CAP + rank] = lists[gid ^ r, listed + t]

            return rank + jnp.where(hit, 1, 0)

        return lax.fori_loop(0, listed, look, carry * 0)

    lax.fori_loop(0, groups, place, 0)
    for q in range(rounds):
        for k in range(slices):
            for c in range(CAP):
                n = (q * slices + (own ^ k)) * CAP + c

                @pl.when(tab[0, n] > 0)
                def _():
                    for start, count, to in slab_pieces(orbs, planes, tab[1, n]):
                        outs[q * slices + k][c, to : to + count, :] = values[pl.ds(start, count, stride=8), :]


def final_kernel(groups, slices, orbs, planes, meta, near_tab, far_tab, values, local_pot, *refs):
    rounds = groups // slices
    nears, fars, out = refs[: rounds * slices], refs[rounds * slices : 2 * rounds * slices], refs[-1]
    own = meta[1]
    out[...] = local_pot[...] * values[...]
    for tab, parts in ((near_tab, nears), (far_tab, fars)):
        for q in range(rounds):
            for k in range(slices):
                for c in range(CAP):
                    n = (q * slices + (own ^ k)) * CAP + c

                    @pl.when(tab[0, n] > 0)
                    def _():
                        for start, count, to in slab_pieces(orbs, planes, tab[1, n]):
                            rows = pl.ds(start, count, stride=8)
                            out[rows, :] = out[rows, :] - parts[q * slices + k][c, to : to + count, :]


def as_rows(x):
    orbs, planes, cells = x.shape
    x = x.transpose(1, 0, 2).reshape(planes, orbs // 8, 8, cells // LANES, LANES)
    return x.transpose(0, 1, 3, 2, 4).reshape(-1, LANES)


def per_device(orbitals, local_pot, pair_owner, pair_remote, pair_resident, pair_count, offsets):
    groups = lax.axis_size("grp")
    slices = lax.axis_size("slc")
    orbs, planes, cells = orbitals.shape
    listed = pair_owner.shape[1]
    rounds = groups // slices
    slab = planes * cells // LANES
    gid = lax.axis_index("grp").astype(jnp.int32)
    sid = lax.axis_index("slc").astype(jnp.int32)
    owner = pair_owner[0, :, 0]
    meta = jnp.concatenate(
        [gid[None], sid[None], owner, pair_remote[0], pair_resident[0], pair_count[0], offsets.reshape(-1)]
    )
    mine = jnp.concatenate([owner, pair_remote[0]])
    lists = lax.all_to_all(jnp.broadcast_to(mine[None], (groups, 2 * listed)), "grp", 0, 0, tiled=True)
    rows = as_rows(orbitals)
    pot_rows = as_rows(local_pot)
    sizes = (groups, slices, listed, orbs, planes)
    tab_shape = jax.ShapeDtypeStruct((5, groups * CAP), jnp.int32)
    packed = pl.pallas_call(
        functools.partial(near_kernel, *sizes),
        in_specs=[smem(), vmem()],
        out_specs=[vmem()] * slices + [smem()],
        out_shape=[jax.ShapeDtypeStruct((rounds * CAP, slab, LANES), jnp.float32)] * slices + [tab_shape],
        scratch_shapes=[pltpu.SMEM((groups,), jnp.int32)],
        name="near_pack",
    )(meta, rows)
    near_tab = packed[slices]
    across = [[(s, s ^ k) for s in range(slices)] for k in range(slices)]
    nears = [packed[0]] + [lax.ppermute(packed[k], "slc", across[k]) for k in range(1, slices)]
    sends = pl.pallas_call(
        functools.partial(far_kernel, *sizes),
        in_specs=[smem(), smem(), vmem()],
        out_specs=[vmem()] * (rounds * slices) + [smem()],
        out_shape=[jax.ShapeDtypeStruct((CAP, slab, LANES), jnp.float32)] * (rounds * slices)
        + [jax.ShapeDtypeStruct((2, groups * CAP), jnp.int32)],
        name="far_pack",
    )(meta, lists, rows)
    far_tab = sends[-1]

    def there(q, k):
        return [
            (g * slices + s, (g ^ (q * slices + (s ^ k))) * slices + (s ^ k))
            for g in range(groups)
            for s in range(slices)
        ]

    consts = make_tables()
    order = list(range(rounds))
    fars = {}
    for q in reversed(order):
        for k in range(slices):
            fars[q, k] = lax.ppermute(sends[q * slices + k], ("grp", "slc"), there(q, k))
    near_back, far_back = {}, {}
    for q in order:
        near_out, far_out = pair_call(
            slices, slab, q, meta, near_tab, nears, [fars[q, k] for k in range(slices)], consts
        )
        for k in range(slices):
            back = [(d, s) for s, d in there(q, k)]
            far_back[q, k] = lax.ppermute(far_out[k], ("grp", "slc"), back)
        for k in range(slices):
            near_back[q, k] = near_out[k] if k == 0 else lax.ppermute(near_out[k], "slc", across[k])
    keys = [(q, k) for q in order for k in range(slices)]
    out = pl.pallas_call(
        functools.partial(final_kernel, groups, slices, orbs, planes),
        in_specs=[smem()] * 3 + [vmem()] * (2 + 2 * len(keys)),
        out_specs=vmem(),
        out_shape=jax.ShapeDtypeStruct(rows.shape, jnp.float32),
        name="gather_fields",
    )(meta, near_tab, far_tab, rows, pot_rows, *[near_back[x] for x in keys], *[far_back[x] for x in keys])
    out = out.reshape(planes, orbs // 8, cells // LANES, 8, LANES).transpose(0, 1, 3, 2, 4)
    return out.reshape(planes, orbs, cells).transpose(1, 0, 2)


def solution(mesh):
    in_specs = (
        P("grp", "slc", None),
        P("grp", "slc", None),
        P("grp", None, None),
        P("grp", None),
        P("grp", None),
        P("grp", None),
        P(),
    )
    return jax.shard_map(
        per_device, mesh=mesh, in_specs=in_specs, out_specs=P("grp", "slc", None), check_vma=False
    )
```

```python
import functools
import jax
import jax.numpy as jnp
import numpy as np
from jax import lax
from jax.experimental import pallas as pl
from jax.experimental.pallas import tpu as pltpu
from jax.sharding import PartitionSpec as P


B = 48
CAP = 2
LANES = 128
COLS = B * B // LANES
BLK = 3 * LANES
ROWS_BLK = BLK // B
NBLK = COLS // 3
PITCH = 56
PAD = (B // 2) * COLS
BOX = B * COLS


def sine_np():
    k = np.arange(B)
    return (np.sqrt(2.0 / (B + 1)) * np.sin(np.pi * (k[:, None] + 1) * (k[None, :] + 1) / (B + 1.0))).astype(
        np.float32
    )


def lam_np():
    k = np.arange(B)
    return 2.0 - 2.0 * np.cos(np.pi * (k + 1.0) / (B + 1.0))


def split(x):
    high = x.astype(jnp.bfloat16)
    return high, (x - high.astype(jnp.float32)).astype(jnp.bfloat16)


def mm(a, b):
    return jnp.dot(a, b, preferred_element_type=jnp.float32)


def mm3(ah, al, bh, bl):
    return mm(ah, bh) + mm(al, bh) + mm(ah, bl)


FWD_K = ((0, 128), (0, 256), (128, 384), (256, 384))


def tables_kernel(sine, wide, lams, after, sine3, fwd_h, fwd_l, inv_h, inv_l, weight):
    q = sine[...]
    qh, ql = split(q)
    q48h, q48l = qh[:, :B], ql[:, :B]
    sine3[...] = jnp.concatenate([q48h, q48h, q48l], axis=1)
    fwd_h[...] = jnp.zeros(fwd_h.shape, jnp.bfloat16)
    fwd_l[...] = jnp.zeros(fwd_l.shape, jnp.bfloat16)
    for b in range(ROWS_BLK):
        fwd_h[b * B : (b + 1) * B, b * LANES : (b + 1) * LANES] = qh
        fwd_l[b * B : (b + 1) * B, b * LANES : (b + 1) * LANES] = ql
    lane = lax.broadcasted_iota(jnp.int32, (LANES, BLK), 1)
    w = jnp.concatenate([wide[...], jnp.zeros((LANES - B, BLK), jnp.float32)], axis=0)
    for b in range(ROWS_BLK):
        part = jnp.where((lane >= b * B) & (lane < (b + 1) * B), w, 0.0)
        ph, plo = split(part)
        inv_h[b * LANES : (b + 1) * LANES, :] = ph
        inv_l[b * LANES : (b + 1) * LANES, :] = plo
    pair = lams[...]
    for k, lam in enumerate(lam_np()):
        weight[:, k * LANES : (k + 1) * LANES] = 1.0 / (pair + np.float32(lam))


def make_tables(after):
    q = sine_np()
    padded = np.zeros((B, LANES), np.float32)
    padded[:, :B] = q
    wide = np.tile(q, (1, ROWS_BLK))
    lam = lam_np()
    lam3 = np.ones((LANES,))
    lam3[:B] = lam
    lams = (lam[:, None] + lam3[None, :]).astype(np.float32)
    wide_shape, tall_shape = (BLK, ROWS_BLK * LANES), (ROWS_BLK * LANES, BLK)
    shapes = (
        pltpu.VMEM((B, 3 * B), jnp.bfloat16),
        pltpu.VMEM(wide_shape, jnp.bfloat16),
        pltpu.VMEM(wide_shape, jnp.bfloat16),
        pltpu.VMEM(tall_shape, jnp.bfloat16),
        pltpu.VMEM(tall_shape, jnp.bfloat16),
        pltpu.VMEM((B, B * LANES), jnp.float32),
    )
    return pl.pallas_call(
        tables_kernel,
        in_specs=[vmem()] * 3 + [smem()],
        out_specs=[vmem()] * len(shapes),
        out_shape=shapes,
        compiler_params=grant(8),
        name="tables",
    )(jnp.asarray(padded), jnp.asarray(wide), jnp.asarray(lams), after)


def one_slot(near, box, shifted, left_h, left_l, mid, mid2, inv_lh, inv_ll, sine3, fwd_h, fwd_l, inv_h, inv_l, weight, spots, out, e0, e1, e2):
    lane = lax.broadcasted_iota(jnp.int32, (B, LANES), 1)

    def turned(source, d0, d1, d2, j_list):
        flat = d0 * (B * B) + d1 * B + d2
        rows = lax.shift_right_arithmetic(flat, 7)
        rest = flat & (LANES - 1)
        back = (LANES - rest) & (LANES - 1)
        rolled = {}
        for j in j_list + [j_list[-1] + 1]:
            rolled[j] = pltpu.roll(source[pl.ds(PAD + rows + j, B, stride=COLS), :], back, axis=1)
        results = []
        for j in j_list:
            moved = jnp.where(lane < LANES - rest, rolled[j], rolled[j + 1])
            bb = spots[j : j + 1, :] + d1
            cc = spots[COLS + j : COLS + j + 1, :] + d2
            inside = (bb >= 0) & (bb < B) & (cc >= 0) & (cc < B)
            results.append(jnp.where(inside, moved, 0.0))
        return results

    s3 = sine3[...]

    def along_first(x):
        xh, xl = split(x)
        return mm(s3, jnp.concatenate([xh, xl, xh], axis=0))

    for m in range(NBLK):
        js = [3 * m, 3 * m + 1, 3 * m + 2]
        parts = turned(box, e0, e1, e2, js)
        dens = []
        for j, part in zip(js, parts):
            shifted[j * B : (j + 1) * B, :] = part
            dens.append(part * near[pl.ds(j, B, stride=COLS), :])
        yh, yl = split(along_first(jnp.concatenate(dens, axis=1)))
        left_h[m * B : (m + 1) * B, :] = yh
        left_l[m * B : (m + 1) * B, :] = yl
    for p, (lo, hi) in enumerate(FWD_K):
        cols = slice(p * 2 * LANES, (p + 1) * 2 * LANES)
        y = mm3(left_h[:, lo:hi], left_l[:, lo:hi], fwd_h[lo:hi, cols], fwd_l[lo:hi, cols])
        for m in range(NBLK):
            for h in range(2):
                b = ROWS_BLK * m + 2 * p + h
                mid[pl.ds(b, B, stride=PITCH), :] = y[m * B : (m + 1) * B, h * LANES : (h + 1) * LANES]
    group = 6

    def second(i, carry):
        first = i * group
        z = jnp.concatenate(
            [mid[pl.ds(pl.multiple_of((first + u) * PITCH, 8), B), :] for u in range(group)], axis=1
        )
        y = along_first(z) * weight[:, pl.ds(pl.multiple_of(first * LANES, LANES), group * LANES)]
        y = along_first(y)
        for u in range(group):
            mid2[pl.ds(first + u, B, stride=PITCH), :] = y[:, u * LANES : (u + 1) * LANES]
        return carry

    lax.fori_loop(0, B // group, second, 0)
    for m in range(NBLK):
        for b in range(ROWS_BLK):
            start = (ROWS_BLK * m + b) * PITCH
            zh, zl = split(mid2[start : start + B, :])
            inv_lh[m * B : (m + 1) * B, b * LANES : (b + 1) * LANES] = zh
            inv_ll[m * B : (m + 1) * B, b * LANES : (b + 1) * LANES] = zl
    ka = slice(0, 6 * LANES)
    kb = slice(5 * LANES, 8 * LANES)
    ya = mm3(inv_lh[:, ka], inv_ll[:, ka], inv_h[ka, : 2 * LANES], inv_l[ka, : 2 * LANES])
    yb = mm3(inv_lh[:, kb], inv_ll[:, kb], inv_h[kb, 2 * LANES :], inv_l[kb, 2 * LANES :])
    for m in range(NBLK):
        y = jnp.concatenate([ya[m * B : (m + 1) * B], yb[m * B : (m + 1) * B]], axis=1)
        pot = along_first(y)
        for u in range(3):
            j = 3 * m + u
            part = pot[:, u * LANES : (u + 1) * LANES]
            box[pl.ds(PAD + j, B, stride=COLS), :] = part * near[pl.ds(j, B, stride=COLS), :]
            out[0, pl.ds(j, B, stride=COLS), :] = part * shifted[j * B : (j + 1) * B, :]
    for m in range(NBLK):
        js = [3 * m, 3 * m + 1, 3 * m + 2]
        for j, part in zip(js, turned(box, -e0, -e1, -e2, js)):
            out[1, pl.ds(j, B, stride=COLS), :] = part


def pair_kernel(slices, slab, round_id, meta, tab, after, *refs):
    nears, refs = refs[:slices], refs[slices:]
    fars, refs = refs[:slices], refs[slices:]
    consts, refs = refs[:7], refs[7:]
    near_outs, refs = refs[:slices], refs[slices:]
    far_outs, refs = refs[:slices], refs[slices:]
    token, refs = refs[0], refs[1:]
    token[0] = after[0]
    near, box, shifted, left_h, left_l, mid, mid2, inv_lh, inv_ll, out = refs
    own = meta[1]
    zeros = jnp.zeros((PAD, LANES), jnp.float32)
    box[:PAD, :] = zeros
    box[PAD + BOX :, :] = zeros
    for c in range(CAP):
        slot = (round_id * slices + own) * CAP + c

        @pl.when(tab[0, slot] > 0)
        def _():
            for k in range(slices):
                start = (own ^ k) * slab
                near[pl.ds(start, slab), :] = nears[k][round_id * CAP + c]
                box[pl.ds(PAD + start, slab), :] = fars[k][c]
            one_slot(near, box, shifted, left_h, left_l, mid, mid2, inv_lh, inv_ll, *consts, out, tab[2, slot], tab[3, slot], tab[4, slot])
            for k in range(slices):
                start = (own ^ k) * slab
                near_outs[k][c] = out[0, pl.ds(start, slab), :]
                far_outs[k][c] = out[1, pl.ds(start, slab), :]


def kept(x):
    return pltpu.with_memory_space_constraint(x, pltpu.VMEM)


def grant(mib):
    return pltpu.CompilerParams(vmem_limit_bytes=mib * 2**20)


def smem():
    return pl.BlockSpec(memory_space=pltpu.SMEM)


def vmem():
    return pl.BlockSpec(memory_space=pltpu.VMEM)


def pair_call(slices, slab, round_id, meta, tab, after, nears, fars, consts):
    spots = np.arange(B * B).reshape(COLS, LANES)
    spots = jnp.asarray(np.concatenate([spots // B, spots % B]).astype(np.int32))
    outs = pl.pallas_call(
        functools.partial(pair_kernel, slices, slab, round_id),
        in_specs=[smem()] * 3 + [vmem()] * (2 * slices + 7),
        out_specs=[vmem()] * (2 * slices) + [smem()],
        out_shape=[pltpu.VMEM((CAP, slab, LANES), jnp.float32)] * (2 * slices) + [jax.ShapeDtypeStruct((1,), jnp.int32)],
        scratch_shapes=[
            pltpu.VMEM((BOX, LANES), jnp.float32),
            pltpu.VMEM((BOX + 2 * PAD, LANES), jnp.float32),
            pltpu.VMEM((BOX, LANES), jnp.float32),
            pltpu.VMEM((NBLK * B, BLK), jnp.bfloat16),
            pltpu.VMEM((NBLK * B, BLK), jnp.bfloat16),
            pltpu.VMEM((B * PITCH, LANES), jnp.float32),
            pltpu.VMEM((B * PITCH, LANES), jnp.float32),
            pltpu.VMEM((NBLK * B, ROWS_BLK * LANES), jnp.bfloat16),
            pltpu.VMEM((NBLK * B, ROWS_BLK * LANES), jnp.bfloat16),
            pltpu.VMEM((2, BOX, LANES), jnp.float32),
        ],
        cost_estimate=pl.CostEstimate(flops=2 * 10**9, transcendentals=0, bytes_accessed=8 * 10**6),
        compiler_params=grant(24),
    )(meta, tab, after, *map(kept, nears), *map(kept, fars), *map(kept, consts), spots)
    return outs[:slices], outs[slices : 2 * slices], outs[-1]


def slab_pieces(orbs, planes, o):
    if orbs == 8:
        return [(o, planes * COLS, 0)]
    tiles = orbs // 8
    high = lax.shift_right_logical(o, 3)
    return [((a * tiles + high) * COLS * 8 + (o & 7), COLS, a * COLS) for a in range(planes)]


def near_kernel(groups, slices, listed, orbs, planes, meta, values, *refs):
    outs, (tab, seen) = refs[:slices], refs[slices:]
    gid = meta[0]
    own = meta[1]
    owner_at, remote_at, resident_at, count_at = 2, 2 + listed, 2 + 2 * listed, 2 + 3 * listed
    offset_at = count_at + slices
    for g in range(groups):
        seen[g] = 0
    for n in range(groups * CAP):
        tab[0, n] = 0

    def place(t, carry):
        running = 0
        home = 0
        for u in range(slices):
            running = running + meta[count_at + u]
            home = home + jnp.where(running <= t, 1, 0)
        owner = meta[owner_at + t]
        rank = seen[owner]
        seen[owner] = rank + 1
        n = (gid ^ owner) * CAP + rank
        local = home * (orbs // slices) + meta[resident_at + t]
        near_at = offset_at + 3 * (gid * orbs + local)
        far_at = offset_at + 3 * (owner * orbs + meta[remote_at + t])
        tab[0, n] = 1
        tab[1, n] = local
        for d in range(3):
            tab[2 + d, n] = meta[near_at + d] - meta[far_at + d]
        return carry

    lax.fori_loop(0, listed, place, 0)
    for k in range(slices):
        for q in range(groups // slices):
            for c in range(CAP):
                n = (q * slices + (own ^ k)) * CAP + c

                @pl.when(tab[0, n] > 0)
                def _():
                    for start, count, to in slab_pieces(orbs, planes, tab[1, n]):
                        outs[k][q * CAP + c, to : to + count, :] = values[pl.ds(start, count, stride=8), :]


def far_kernel(groups, slices, listed, orbs, planes, lists, values, *refs):
    rounds = groups // slices
    outs, (tab, after) = refs[: rounds * slices], refs[rounds * slices :]
    gid = lists[0, 2 * listed]
    own = lists[0, 2 * listed + 1]
    after[0] = own
    for n in range(groups * CAP):
        tab[0, n] = 0

    def place(r, carry):
        def look(t, rank):
            hit = lists[gid ^ r, t] == gid

            @pl.when(hit)
            def _():
                tab[0, r * CAP + rank] = 1
                tab[1, r * CAP + rank] = lists[gid ^ r, listed + t]

            return rank + jnp.where(hit, 1, 0)

        return lax.fori_loop(0, listed, look, carry * 0)

    lax.fori_loop(0, groups, place, 0)
    for q in range(rounds):
        for k in range(slices):
            for c in range(CAP):
                n = (q * slices + (own ^ k)) * CAP + c

                @pl.when(tab[0, n] > 0)
                def _():
                    for start, count, to in slab_pieces(orbs, planes, tab[1, n]):
                        outs[q * slices + k][c, to : to + count, :] = values[pl.ds(start, count, stride=8), :]


def sum_kernel(slices, orbs, planes, rounds, first, meta, near_tab, far_tab, base, *refs):
    if first:
        values, refs = refs[0], refs[1:]
    count = len(rounds) * slices
    nears, fars, out = refs[:count], refs[count : 2 * count], refs[-1]
    own = meta[1]
    out[...] = base[...] * values[...] if first else base[...]
    for tab, parts in ((near_tab, nears), (far_tab, fars)):
        for at, q in enumerate(rounds):
            for k in range(slices):
                for c in range(CAP):
                    n = (q * slices + (own ^ k)) * CAP + c

                    @pl.when(tab[0, n] > 0)
                    def _():
                        for start, count, to in slab_pieces(orbs, planes, tab[1, n]):
                            rows = pl.ds(start, count, stride=8)
                            out[rows, :] = out[rows, :] - parts[at * slices + k][c, to : to + count, :]


def as_rows(x):
    orbs, planes, cells = x.shape
    x = x.transpose(1, 0, 2).reshape(planes, orbs // 8, 8, cells // LANES, LANES)
    return x.transpose(0, 1, 3, 2, 4).reshape(-1, LANES)


def operator(orbitals, local_pot, pair_owner, pair_remote, pair_resident, pair_count, offsets):
    groups = lax.axis_size("grp")
    slices = lax.axis_size("slc")
    orbs, planes, cells = orbitals.shape
    listed = pair_owner.shape[1]
    rounds = groups // slices
    slab = planes * cells // LANES
    gid = lax.axis_index("grp").astype(jnp.int32)
    sid = lax.axis_index("slc").astype(jnp.int32)
    owner = pair_owner[0, :, 0]
    meta = jnp.concatenate(
        [gid[None], sid[None], owner, pair_remote[0], pair_resident[0], pair_count[0], offsets.reshape(-1)]
    )
    where = lax.broadcasted_iota(jnp.int32, (groups, 2), 0)
    where = jnp.where(lax.broadcasted_iota(jnp.int32, (groups, 2), 1) == 0, where, sid)
    mine = jnp.concatenate([owner, pair_remote[0]])
    mine = jnp.concatenate([jnp.broadcast_to(mine[None], (groups, 2 * listed)), where], axis=1)
    lists = lax.all_to_all(mine, "grp", 0, 0, tiled=True)
    rows = as_rows(orbitals)
    pot_rows = as_rows(local_pot)
    sizes = (groups, slices, listed, orbs, planes)
    keys = [(q, k) for q in range(rounds) for k in range(slices)]
    word = jax.ShapeDtypeStruct((1,), jnp.int32)
    packed = pl.pallas_call(
        functools.partial(near_kernel, *sizes),
        in_specs=[smem(), vmem()],
        out_specs=[vmem()] * slices + [smem()],
        out_shape=[pltpu.VMEM((rounds * CAP, slab, LANES), jnp.float32)] * slices
        + [jax.ShapeDtypeStruct((5, groups * CAP), jnp.int32)],
        scratch_shapes=[pltpu.SMEM((groups,), jnp.int32)],
        compiler_params=grant(4),
        name="near_pack",
    )(meta, rows)
    near_tab = packed[slices]
    across = [[(s, s ^ k) for s in range(slices)] for k in range(slices)]
    nears = [packed[0]]
    for k in range(1, slices):
        nears.append(lax.ppermute(packed[k], "slc", across[k]))
    sends = pl.pallas_call(
        functools.partial(far_kernel, *sizes),
        in_specs=[smem(), vmem()],
        out_specs=[vmem()] * len(keys) + [smem()] * 2,
        out_shape=[pltpu.VMEM((CAP, slab, LANES), jnp.float32)] * len(keys)
        + [jax.ShapeDtypeStruct((2, groups * CAP), jnp.int32), word],
        compiler_params=grant(4),
        name="far_pack",
    )(lists, rows)
    far_tab, after = sends[-2], sends[-1]

    def there(q, k):
        return [
            (g * slices + s, (g ^ (q * slices + (s ^ k))) * slices + (s ^ k))
            for g in range(groups)
            for s in range(slices)
        ]

    fars = {}
    for q, k in keys:
        fars[q, k] = lax.ppermute(sends[q * slices + k], ("grp", "slc"), there(q, k))
    consts = make_tables(after)
    near_back, far_back = {}, {}
    for q in range(rounds):
        near_out, far_out, after = pair_call(
            slices, slab, q, meta, near_tab, after, nears, [fars[q, k] for k in range(slices)], consts
        )
        for k in range(slices):
            back = [(d, s) for s, d in there(q, k)]
            far_back[q, k] = lax.ppermute(far_out[k], ("grp", "slc"), back)
            near_back[q, k] = near_out[k] if k == 0 else lax.ppermute(near_out[k], "slc", across[k])
    out = None
    for chosen in (tuple(range(rounds - 1)), (rounds - 1,)):
        first = out is None
        base = [pot_rows, rows] if first else [out]
        part = [x for x in keys if x[0] in chosen]
        parts = [kept(near_back[x]) for x in part] + [kept(far_back[x]) for x in part]
        out = pl.pallas_call(
            functools.partial(sum_kernel, slices, orbs, planes, chosen, first),
            in_specs=[smem()] * 3 + [vmem()] * (len(base) + len(parts)),
            out_specs=vmem(),
            out_shape=jax.ShapeDtypeStruct(rows.shape, jnp.float32),
            input_output_aliases={} if first else {3: 0},
            compiler_params=grant(6),
        )(meta, near_tab, far_tab, *base, *parts)
    out = out.reshape(planes, orbs // 8, cells // LANES, 8, LANES).transpose(0, 1, 3, 2, 4)
    return out.reshape(planes, orbs, cells).transpose(1, 0, 2)


def solution(mesh):
    in_specs = (
        P("grp", "slc", None),
        P("grp", "slc", None),
        P("grp", None, None),
        P("grp", None),
        P("grp", None),
        P("grp", None),
        P(),
    )
    return jax.shard_map(operator, mesh=mesh, in_specs=in_specs, out_specs=P("grp", "slc", None), check_vma=False)
```

```python
import functools
import jax
import jax.numpy as jnp
import numpy as np
from jax import lax
from jax.experimental import pallas as pl
from jax.experimental.pallas import tpu as pltpu
from jax.sharding import PartitionSpec as P


B = 48
CAP = 2
LANES = 128
COLS = B * B // LANES
BLK = 3 * LANES
ROWS_BLK = BLK // B
NBLK = COLS // 3
PITCH = 56
PAD = (B // 2) * COLS
BOX = B * COLS


def sine_np():
    k = np.arange(B)
    return (np.sqrt(2.0 / (B + 1)) * np.sin(np.pi * (k[:, None] + 1) * (k[None, :] + 1) / (B + 1.0))).astype(
        np.float32
    )


def lam_np():
    k = np.arange(B)
    return 2.0 - 2.0 * np.cos(np.pi * (k + 1.0) / (B + 1.0))


def split(x):
    high = x.astype(jnp.bfloat16)
    return high, (x - high.astype(jnp.float32)).astype(jnp.bfloat16)


def mm(a, b):
    return jnp.dot(a, b, preferred_element_type=jnp.float32)


def mm3(ah, al, bh, bl):
    return mm(ah, bh) + mm(al, bh) + mm(ah, bl)


FWD_K = ((0, 128), (0, 256), (128, 384), (256, 384))


def tables_kernel(sine, wide, lams, after, sine3, fwd_h, fwd_l, inv_h, inv_l, weight):
    q = sine[...]
    qh, ql = split(q)
    q48h, q48l = qh[:, :B], ql[:, :B]
    sine3[...] = jnp.concatenate([q48h, q48h, q48l], axis=1)
    fwd_h[...] = jnp.zeros(fwd_h.shape, jnp.bfloat16)
    fwd_l[...] = jnp.zeros(fwd_l.shape, jnp.bfloat16)
    for b in range(ROWS_BLK):
        fwd_h[b * B : (b + 1) * B, b * LANES : (b + 1) * LANES] = qh
        fwd_l[b * B : (b + 1) * B, b * LANES : (b + 1) * LANES] = ql
    lane = lax.broadcasted_iota(jnp.int32, (LANES, BLK), 1)
    w = jnp.concatenate([wide[...], jnp.zeros((LANES - B, BLK), jnp.float32)], axis=0)
    for b in range(ROWS_BLK):
        part = jnp.where((lane >= b * B) & (lane < (b + 1) * B), w, 0.0)
        ph, plo = split(part)
        half = ph[: LANES // 2]
        inv_h[b * LANES : (b + 1) * LANES, :] = jnp.concatenate([half, half], axis=0)
        inv_l[b * LANES : (b + 1) * LANES, :] = plo
    pair = lams[...]
    for k, lam in enumerate(lam_np()):
        weight[:, k * LANES : (k + 1) * LANES] = 1.0 / (pair + np.float32(lam))


def make_tables(after):
    q = sine_np()
    padded = np.zeros((B, LANES), np.float32)
    padded[:, :B] = q
    wide = np.tile(q, (1, ROWS_BLK))
    lam = lam_np()
    lam3 = np.ones((LANES,))
    lam3[:B] = lam
    lams = (lam[:, None] + lam3[None, :]).astype(np.float32)
    wide_shape, tall_shape = (BLK, ROWS_BLK * LANES), (ROWS_BLK * LANES, BLK)
    shapes = (
        pltpu.VMEM((B, 3 * B), jnp.bfloat16),
        pltpu.VMEM(wide_shape, jnp.bfloat16),
        pltpu.VMEM(wide_shape, jnp.bfloat16),
        pltpu.VMEM(tall_shape, jnp.bfloat16),
        pltpu.VMEM(tall_shape, jnp.bfloat16),
        pltpu.VMEM((B, B * LANES), jnp.float32),
    )
    return pl.pallas_call(
        tables_kernel,
        in_specs=[vmem()] * 3 + [smem()],
        out_specs=[vmem()] * len(shapes),
        out_shape=shapes,
        compiler_params=grant(8),
        name="tables",
    )(jnp.asarray(padded), jnp.asarray(wide), jnp.asarray(lams), after)


def one_slot(near, box, shifted, left_h, left_l, mid, mid2, inv_left, sine3, fwd_h, fwd_l, inv_h, inv_l, weight, spots, out, e0, e1, e2):
    lane = lax.broadcasted_iota(jnp.int32, (B, LANES), 1)

    def turned(source, d0, d1, d2, j_list):
        flat = d0 * (B * B) + d1 * B + d2
        rows = lax.shift_right_arithmetic(flat, 7)
        rest = flat & (LANES - 1)
        back = (LANES - rest) & (LANES - 1)
        rolled = {}
        for j in j_list + [j_list[-1] + 1]:
            rolled[j] = pltpu.roll(source[pl.ds(PAD + rows + j, B, stride=COLS), :], back, axis=1)
        results = []
        for j in j_list:
            moved = jnp.where(lane < LANES - rest, rolled[j], rolled[j + 1])
            bb = spots[j : j + 1, :] + d1
            cc = spots[COLS + j : COLS + j + 1, :] + d2
            inside = (bb >= 0) & (bb < B) & (cc >= 0) & (cc < B)
            results.append(jnp.where(inside, moved, 0.0))
        return results

    s3 = sine3[...]

    def along_first(x):
        xh, xl = split(x)
        return mm(s3, jnp.concatenate([xh, xl, xh], axis=0))

    for m in range(NBLK):
        js = [3 * m, 3 * m + 1, 3 * m + 2]
        parts = turned(box, e0, e1, e2, js)
        dens = []
        for j, part in zip(js, parts):
            shifted[j * B : (j + 1) * B, :] = part
            dens.append(part * near[pl.ds(j, B, stride=COLS), :])
        yh, yl = split(along_first(jnp.concatenate(dens, axis=1)))
        left_h[m * B : (m + 1) * B, :] = yh
        left_l[m * B : (m + 1) * B, :] = yl
    for p, (lo, hi) in enumerate(FWD_K):
        cols = slice(p * 2 * LANES, (p + 1) * 2 * LANES)
        y = mm3(left_h[:, lo:hi], left_l[:, lo:hi], fwd_h[lo:hi, cols], fwd_l[lo:hi, cols])
        for m in range(NBLK):
            for h in range(2):
                b = ROWS_BLK * m + 2 * p + h
                mid[pl.ds(b, B, stride=PITCH), :] = y[m * B : (m + 1) * B, h * LANES : (h + 1) * LANES]
    group = 48

    def second(i, carry):
        first = i * group
        z = jnp.concatenate(
            [mid[pl.ds(pl.multiple_of((first + u) * PITCH, 8), B), :] for u in range(group)], axis=1
        )
        y = along_first(z) * weight[:, pl.ds(pl.multiple_of(first * LANES, LANES), group * LANES)]
        y = along_first(y)
        for u in range(group):
            mid2[pl.ds(first + u, B, stride=PITCH), :] = y[:, u * LANES : (u + 1) * LANES]
        return carry

    lax.fori_loop(0, B // group, second, 0)
    for m in range(NBLK):
        for b in range(ROWS_BLK):
            start = (ROWS_BLK * m + b) * PITCH
            z = mid2[start : start + B, :]
            zh = z.astype(jnp.bfloat16).astype(jnp.float32)
            both = zh + pltpu.roll(z - zh, LANES // 2, axis=1)
            inv_left[m * B : (m + 1) * B, b * LANES : (b + 1) * LANES] = both.astype(jnp.bfloat16)
    ka = slice(0, 6 * LANES)
    kb = slice(5 * LANES, 8 * LANES)
    ya = mm(inv_left[:, ka], inv_h[ka, : 2 * LANES]) + mm(inv_left[:, ka], inv_l[ka, : 2 * LANES])
    yb = mm(inv_left[:, kb], inv_h[kb, 2 * LANES :]) + mm(inv_left[:, kb], inv_l[kb, 2 * LANES :])
    for m in range(NBLK):
        y = jnp.concatenate([ya[m * B : (m + 1) * B], yb[m * B : (m + 1) * B]], axis=1)
        pot = along_first(y)
        for u in range(3):
            j = 3 * m + u
            part = pot[:, u * LANES : (u + 1) * LANES]
            box[pl.ds(PAD + j, B, stride=COLS), :] = part * near[pl.ds(j, B, stride=COLS), :]
            out[0, pl.ds(j, B, stride=COLS), :] = part * shifted[j * B : (j + 1) * B, :]
    for m in range(NBLK):
        js = [3 * m, 3 * m + 1, 3 * m + 2]
        for j, part in zip(js, turned(box, -e0, -e1, -e2, js)):
            out[1, pl.ds(j, B, stride=COLS), :] = part


def pair_kernel(slices, slab, round_id, ranks, tab, *refs):
    nears, refs = refs[:slices], refs[slices:]
    fars, refs = refs[:slices], refs[slices:]
    consts, refs = refs[:7], refs[7:]
    if ranks[0]:
        refs = refs[slices:]
    near_outs, refs = refs[:slices], refs[slices:]
    far_outs, refs = refs[:slices], refs[slices:]
    near, box, shifted, left_h, left_l, mid, mid2, inv_left, out = refs
    own = tab[5, 0]
    zeros = jnp.zeros((PAD, LANES), jnp.float32)
    box[:PAD, :] = zeros
    box[PAD + BOX :, :] = zeros
    for at, c in enumerate(ranks):
        slot = (round_id * slices + own) * CAP + c

        @pl.when(tab[0, slot] > 0)
        def _():
            for k in range(slices):
                start = (own ^ k) * slab
                near[pl.ds(start, slab), :] = nears[k][c]
                box[pl.ds(PAD + start, slab), :] = fars[k][c]
            one_slot(near, box, shifted, left_h, left_l, mid, mid2, inv_left, *consts, out, tab[2, slot], tab[3, slot], tab[4, slot])
            for k in range(slices):
                start = (own ^ k) * slab
                near_outs[k][c] = out[0, pl.ds(start, slab), :]
                far_outs[k][at] = out[1, pl.ds(start, slab), :]


def kept(x):
    return pltpu.with_memory_space_constraint(x, pltpu.VMEM)


def grant(mib):
    return pltpu.CompilerParams(vmem_limit_bytes=mib * 2**20)


def smem():
    return pl.BlockSpec(memory_space=pltpu.SMEM)


def vmem():
    return pl.BlockSpec(memory_space=pltpu.VMEM)


def pair_call(slices, slab, round_id, ranks, tab, nears, fars, consts, earlier):
    spots = np.arange(B * B).reshape(COLS, LANES)
    spots = jnp.asarray(np.concatenate([spots // B, spots % B]).astype(np.int32))
    operands = [tab, *map(kept, nears), *map(kept, fars), *map(kept, consts), spots, *map(kept, earlier)]
    outs = pl.pallas_call(
        functools.partial(pair_kernel, slices, slab, round_id, ranks),
        in_specs=[smem()] + [vmem()] * (len(operands) - 1),
        out_specs=[vmem()] * (2 * slices),
        out_shape=[pltpu.VMEM((CAP, slab, LANES), jnp.float32)] * slices
        + [pltpu.VMEM((len(ranks), slab, LANES), jnp.float32)] * slices,
        input_output_aliases={len(operands) - len(earlier) + k: k for k in range(len(earlier))},
        scratch_shapes=[
            pltpu.VMEM((BOX, LANES), jnp.float32),
            pltpu.VMEM((BOX + 2 * PAD, LANES), jnp.float32),
            pltpu.VMEM((BOX, LANES), jnp.float32),
            pltpu.VMEM((NBLK * B, BLK), jnp.bfloat16),
            pltpu.VMEM((NBLK * B, BLK), jnp.bfloat16),
            pltpu.VMEM((B * PITCH, LANES), jnp.float32),
            pltpu.VMEM((B * PITCH, LANES), jnp.float32),
            pltpu.VMEM((NBLK * B, ROWS_BLK * LANES), jnp.bfloat16),
            pltpu.VMEM((2, BOX, LANES), jnp.float32),
        ],
        cost_estimate=pl.CostEstimate(flops=2 * 10**9, transcendentals=0, bytes_accessed=8 * 10**6),
        compiler_params=grant(24),
    )(*operands)
    return outs[:slices], outs[slices:]


def slab_pieces(orbs, planes, o):
    if orbs == 8:
        return [(o, planes * COLS, 0)]
    tiles = orbs // 8
    high = lax.shift_right_logical(o, 3)
    return [((a * tiles + high) * COLS * 8 + (o & 7), COLS, a * COLS) for a in range(planes)]


def near_kernel(groups, slices, listed, orbs, planes, meta, values, *refs):
    rounds = groups // slices
    outs, (tab, seen) = refs[: rounds * slices], refs[rounds * slices :]
    gid = meta[0]
    own = meta[1]
    tab[5, 0] = own
    owner_at, remote_at, resident_at, count_at = 2, 2 + listed, 2 + 2 * listed, 2 + 3 * listed
    offset_at = count_at + slices
    for g in range(groups):
        seen[g] = 0
    for n in range(groups * CAP):
        tab[0, n] = 0

    def place(t, carry):
        running = 0
        home = 0
        for u in range(slices):
            running = running + meta[count_at + u]
            home = home + jnp.where(running <= t, 1, 0)
        owner = meta[owner_at + t]
        rank = seen[owner]
        seen[owner] = rank + 1
        n = (gid ^ owner) * CAP + rank
        local = home * (orbs // slices) + meta[resident_at + t]
        near_at = offset_at + 3 * (gid * orbs + local)
        far_at = offset_at + 3 * (owner * orbs + meta[remote_at + t])
        tab[0, n] = 1
        tab[1, n] = local
        for d in range(3):
            tab[2 + d, n] = meta[near_at + d] - meta[far_at + d]
        return carry

    lax.fori_loop(0, listed, place, 0)
    for q in range(rounds):
        for k in range(slices):
            for c in range(CAP):
                n = (q * slices + (own ^ k)) * CAP + c

                @pl.when(tab[0, n] > 0)
                def _():
                    for start, count, to in slab_pieces(orbs, planes, tab[1, n]):
                        outs[q * slices + k][c, to : to + count, :] = values[pl.ds(start, count, stride=8), :]


def far_kernel(groups, slices, listed, orbs, planes, lists, values, *refs):
    rounds = groups // slices
    outs, (tab, after) = refs[: rounds * slices], refs[rounds * slices :]
    gid = lists[0, 2 * listed]
    own = lists[0, 2 * listed + 1]
    after[0] = own
    for n in range(groups * CAP):
        tab[0, n] = 0

    def place(r, carry):
        def look(t, rank):
            hit = lists[gid ^ r, t] == gid

            @pl.when(hit)
            def _():
                tab[0, r * CAP + rank] = 1
                tab[1, r * CAP + rank] = lists[gid ^ r, listed + t]

            return rank + jnp.where(hit, 1, 0)

        return lax.fori_loop(0, listed, look, carry * 0)

    lax.fori_loop(0, groups, place, 0)
    for q in range(rounds):
        for k in range(slices):
            for c in range(CAP):
                n = (q * slices + (own ^ k)) * CAP + c

                @pl.when(tab[0, n] > 0)
                def _():
                    for start, count, to in slab_pieces(orbs, planes, tab[1, n]):
                        outs[q * slices + k][c, to : to + count, :] = values[pl.ds(start, count, stride=8), :]


def sum_kernel(slices, orbs, planes, near_keys, far_keys, first, near_tab, far_tab, base, *refs):
    if first:
        values, refs = refs[0], refs[1:]
    out = refs[-1]
    own = near_tab[5, 0]
    out[...] = base[...] * values[...] if first else base[...]
    for tab, keys, parts in ((near_tab, near_keys, refs), (far_tab, far_keys, refs[len(near_keys) :])):
        for part, (q, k, ranks) in zip(parts, keys):
            for at, c in enumerate(ranks):
                n = (q * slices + (own ^ k)) * CAP + c

                @pl.when(tab[0, n] > 0)
                def _():
                    for start, count, to in slab_pieces(orbs, planes, tab[1, n]):
                        rows = pl.ds(start, count, stride=8)
                        out[rows, :] = out[rows, :] - part[at, to : to + count, :]


def as_rows(x):
    orbs, planes, cells = x.shape
    x = x.transpose(1, 0, 2).reshape(planes, orbs // 8, 8, cells // LANES, LANES)
    return x.transpose(0, 1, 3, 2, 4).reshape(-1, LANES)


def operator(orbitals, local_pot, pair_owner, pair_remote, pair_resident, pair_count, offsets):
    groups = lax.axis_size("grp")
    slices = lax.axis_size("slc")
    orbs, planes, cells = orbitals.shape
    listed = pair_owner.shape[1]
    rounds = groups // slices
    slab = planes * cells // LANES
    gid = lax.axis_index("grp").astype(jnp.int32)
    sid = lax.axis_index("slc").astype(jnp.int32)
    owner = pair_owner[0, :, 0]
    meta = jnp.concatenate(
        [gid[None], sid[None], owner, pair_remote[0], pair_resident[0], pair_count[0], offsets.reshape(-1)]
    )
    where = lax.broadcasted_iota(jnp.int32, (groups, 2), 0)
    where = jnp.where(lax.broadcasted_iota(jnp.int32, (groups, 2), 1) == 0, where, sid)
    mine = jnp.concatenate([owner, pair_remote[0]])
    mine = jnp.concatenate([jnp.broadcast_to(mine[None], (groups, 2 * listed)), where], axis=1)
    lists = lax.all_to_all(mine, "grp", 0, 0, tiled=True)
    rows = as_rows(orbitals)
    pot_rows = as_rows(local_pot)
    sizes = (groups, slices, listed, orbs, planes)
    keys = [(q, k) for q in range(rounds) for k in range(slices)]
    word = jax.ShapeDtypeStruct((1,), jnp.int32)
    packed = pl.pallas_call(
        functools.partial(near_kernel, *sizes),
        in_specs=[smem(), vmem()],
        out_specs=[vmem()] * len(keys) + [smem()],
        out_shape=[pltpu.VMEM((CAP, slab, LANES), jnp.float32)] * len(keys)
        + [jax.ShapeDtypeStruct((6, groups * CAP), jnp.int32)],
        scratch_shapes=[pltpu.SMEM((groups,), jnp.int32)],
        compiler_params=grant(4),
        name="near_pack",
    )(meta, rows)
    near_tab = packed[-1]
    across = [[(s, s ^ k) for s in range(slices)] for k in range(slices)]
    nears = {}
    for q, k in keys:
        nears[q, k] = packed[q * slices + k]
        if k:
            nears[q, k] = lax.ppermute(nears[q, k], "slc", across[k])
    sends = pl.pallas_call(
        functools.partial(far_kernel, *sizes),
        in_specs=[smem(), vmem()],
        out_specs=[vmem()] * len(keys) + [smem()] * 2,
        out_shape=[pltpu.VMEM((CAP, slab, LANES), jnp.float32)] * len(keys)
        + [jax.ShapeDtypeStruct((2, groups * CAP), jnp.int32), word],
        compiler_params=grant(4),
        name="far_pack",
    )(lists, rows)
    far_tab, after = sends[-2], sends[-1]

    def there(q, k):
        return [
            (g * slices + s, (g ^ (q * slices + (s ^ k))) * slices + (s ^ k))
            for g in range(groups)
            for s in range(slices)
        ]

    fars = {}
    for q, k in keys:
        fars[q, k] = lax.ppermute(sends[q * slices + k], ("grp", "slc"), there(q, k))
    consts = make_tables(after)
    every = tuple(range(CAP))
    near_back, far_back = {}, {}
    for q in range(rounds):
        earlier = []
        for ranks in rank_sets(q, rounds):
            earlier, far_out = pair_call(
                slices, slab, q, ranks, near_tab, [nears[q, k] for k in range(slices)],
                [fars[q, k] for k in range(slices)], consts, earlier
            )
            for k in range(slices):
                back = [(d, s) for s, d in there(q, k)]
                far_back[q, k, ranks] = lax.ppermute(far_out[k], ("grp", "slc"), back)
        for k in range(slices):
            near_back[q, k, every] = earlier[k] if k == 0 else lax.ppermute(earlier[k], "slc", across[k])
    out = None
    for chosen in (tuple(range(rounds - 1)), (rounds - 1,)):
        first = out is None
        base = [pot_rows, rows] if first else [out]
        near_keys = [x for x in near_back if x[0] in chosen]
        far_keys = [x for x in far_back if x[0] in chosen]
        parts = [kept(near_back[x]) for x in near_keys] + [kept(far_back[x]) for x in far_keys]
        out = pl.pallas_call(
            functools.partial(sum_kernel, slices, orbs, planes, near_keys, far_keys, first),
            in_specs=[smem()] * 2 + [vmem()] * (len(base) + len(parts)),
            out_specs=vmem(),
            out_shape=jax.ShapeDtypeStruct(rows.shape, jnp.float32),
            input_output_aliases={} if first else {2: 0},
            compiler_params=grant(6),
        )(near_tab, far_tab, *base, *parts)
    out = out.reshape(planes, orbs // 8, cells // LANES, 8, LANES).transpose(0, 1, 3, 2, 4)
    return out.reshape(planes, orbs, cells).transpose(1, 0, 2)


def rank_sets(q, rounds):
    return [(c,) for c in range(CAP)] if q == rounds - 1 else [tuple(range(CAP))]


def solution(mesh):
    in_specs = (
        P("grp", "slc", None),
        P("grp", "slc", None),
        P("grp", None, None),
        P("grp", None),
        P("grp", None),
        P("grp", None),
        P(),
    )
    return jax.shard_map(operator, mesh=mesh, in_specs=in_specs, out_specs=P("grp", "slc", None), check_vma=False)
```

```python
import functools
import jax
import jax.numpy as jnp
import numpy as np
from jax import lax
from jax.experimental import pallas as pl
from jax.experimental.pallas import tpu as pltpu
from jax.sharding import PartitionSpec as P


B = 48
CAP = 2
LANES = 128
COLS = B * B // LANES
BLK = 3 * LANES
ROWS_BLK = BLK // B
NBLK = COLS // 3
PITCH = 56
PAD = (B // 2) * COLS
BOX = B * COLS


def sine_np():
    k = np.arange(B)
    return (np.sqrt(2.0 / (B + 1)) * np.sin(np.pi * (k[:, None] + 1) * (k[None, :] + 1) / (B + 1.0))).astype(
        np.float32
    )


def lam_np():
    k = np.arange(B)
    return 2.0 - 2.0 * np.cos(np.pi * (k + 1.0) / (B + 1.0))


def split(x):
    high = x.astype(jnp.bfloat16)
    return high, (x - high.astype(jnp.float32)).astype(jnp.bfloat16)


def mm(a, b):
    return jnp.dot(a, b, preferred_element_type=jnp.float32)


def mm3(ah, al, bh, bl):
    return mm(ah, bh) + mm(al, bh) + mm(ah, bl)


FWD_K = ((0, 128), (0, 256), (128, 384), (256, 384))


def tables_kernel(sine, wide, lams, after, sine3, fwd_h, fwd_l, inv_h, inv_l, weight):
    q = sine[...]
    qh, ql = split(q)
    q48h, q48l = qh[:, :B], ql[:, :B]
    sine3[...] = jnp.concatenate([q48h, q48h, q48l], axis=1)
    fwd_h[...] = jnp.zeros(fwd_h.shape, jnp.bfloat16)
    fwd_l[...] = jnp.zeros(fwd_l.shape, jnp.bfloat16)
    for b in range(ROWS_BLK):
        fwd_h[b * B : (b + 1) * B, b * LANES : (b + 1) * LANES] = qh
        fwd_l[b * B : (b + 1) * B, b * LANES : (b + 1) * LANES] = ql
    lane = lax.broadcasted_iota(jnp.int32, (LANES, BLK), 1)
    w = jnp.concatenate([wide[...], jnp.zeros((LANES - B, BLK), jnp.float32)], axis=0)
    for b in range(ROWS_BLK):
        part = jnp.where((lane >= b * B) & (lane < (b + 1) * B), w, 0.0)
        ph, plo = split(part)
        half = ph[: LANES // 2]
        inv_h[b * LANES : (b + 1) * LANES, :] = jnp.concatenate([half, half], axis=0)
        inv_l[b * LANES : (b + 1) * LANES, :] = plo
    pair = lams[...]
    for k, lam in enumerate(lam_np()):
        weight[:, k * LANES : (k + 1) * LANES] = 1.0 / (pair + np.float32(lam))


def make_tables(after):
    q = sine_np()
    padded = np.zeros((B, LANES), np.float32)
    padded[:, :B] = q
    wide = np.tile(q, (1, ROWS_BLK))
    lam = lam_np()
    lam3 = np.ones((LANES,))
    lam3[:B] = lam
    lams = (lam[:, None] + lam3[None, :]).astype(np.float32)
    wide_shape, tall_shape = (BLK, ROWS_BLK * LANES), (ROWS_BLK * LANES, BLK)
    shapes = (
        pltpu.VMEM((B, 3 * B), jnp.bfloat16),
        pltpu.VMEM(wide_shape, jnp.bfloat16),
        pltpu.VMEM(wide_shape, jnp.bfloat16),
        pltpu.VMEM(tall_shape, jnp.bfloat16),
        pltpu.VMEM(tall_shape, jnp.bfloat16),
        pltpu.VMEM((B, B * LANES), jnp.float32),
    )
    return pl.pallas_call(
        tables_kernel,
        in_specs=[vmem()] * 3 + [smem()],
        out_specs=[vmem()] * len(shapes),
        out_shape=shapes,
        compiler_params=grant(8),
        name="tables",
    )(jnp.asarray(padded), jnp.asarray(wide), jnp.asarray(lams), after)


def one_slot(near, box, shifted, left_h, left_l, mid, mid2, inv_left, sine3, fwd_h, fwd_l, inv_h, inv_l, weight, spots, out, e0, e1, e2):
    lane = lax.broadcasted_iota(jnp.int32, (B, LANES), 1)

    def turned(source, d0, d1, d2, j_list):
        flat = d0 * (B * B) + d1 * B + d2
        rows = lax.shift_right_arithmetic(flat, 7)
        rest = flat & (LANES - 1)
        back = (LANES - rest) & (LANES - 1)
        rolled = {}
        for j in j_list + [j_list[-1] + 1]:
            rolled[j] = pltpu.roll(source[pl.ds(PAD + rows + j, B, stride=COLS), :], back, axis=1)
        results = []
        for j in j_list:
            moved = jnp.where(lane < LANES - rest, rolled[j], rolled[j + 1])
            bb = spots[j : j + 1, :] + d1
            cc = spots[COLS + j : COLS + j + 1, :] + d2
            inside = (bb >= 0) & (bb < B) & (cc >= 0) & (cc < B)
            results.append(jnp.where(inside, moved, 0.0))
        return results

    s3 = sine3[...]

    def along_first(x):
        xh, xl = split(x)
        return mm(s3, jnp.concatenate([xh, xl, xh], axis=0))

    for m in range(NBLK):
        js = [3 * m, 3 * m + 1, 3 * m + 2]
        parts = turned(box, e0, e1, e2, js)
        dens = []
        for j, part in zip(js, parts):
            shifted[j * B : (j + 1) * B, :] = part
            dens.append(part * near[pl.ds(j, B, stride=COLS), :])
        yh, yl = split(along_first(jnp.concatenate(dens, axis=1)))
        left_h[m * B : (m + 1) * B, :] = yh
        left_l[m * B : (m + 1) * B, :] = yl
    for p, (lo, hi) in enumerate(FWD_K):
        cols = slice(p * 2 * LANES, (p + 1) * 2 * LANES)
        y = mm3(left_h[:, lo:hi], left_l[:, lo:hi], fwd_h[lo:hi, cols], fwd_l[lo:hi, cols])
        for m in range(NBLK):
            for h in range(2):
                b = ROWS_BLK * m + 2 * p + h
                mid[pl.ds(b, B, stride=PITCH), :] = y[m * B : (m + 1) * B, h * LANES : (h + 1) * LANES]
    group = 48

    def second(i, carry):
        first = i * group
        z = jnp.concatenate(
            [mid[pl.ds(pl.multiple_of((first + u) * PITCH, 8), B), :] for u in range(group)], axis=1
        )
        y = along_first(z) * weight[:, pl.ds(pl.multiple_of(first * LANES, LANES), group * LANES)]
        y = along_first(y)
        for u in range(group):
            mid2[pl.ds(first + u, B, stride=PITCH), :] = y[:, u * LANES : (u + 1) * LANES]
        return carry

    lax.fori_loop(0, B // group, second, 0)
    for m in range(NBLK):
        for b in range(ROWS_BLK):
            start = (ROWS_BLK * m + b) * PITCH
            z = mid2[start : start + B, :]
            zh = z.astype(jnp.bfloat16).astype(jnp.float32)
            both = zh + pltpu.roll(z - zh, LANES // 2, axis=1)
            inv_left[m * B : (m + 1) * B, b * LANES : (b + 1) * LANES] = both.astype(jnp.bfloat16)
    ka = slice(0, 6 * LANES)
    kb = slice(5 * LANES, 8 * LANES)
    ya = mm(inv_left[:, ka], inv_h[ka, : 2 * LANES]) + mm(inv_left[:, ka], inv_l[ka, : 2 * LANES])
    yb = mm(inv_left[:, kb], inv_h[kb, 2 * LANES :]) + mm(inv_left[:, kb], inv_l[kb, 2 * LANES :])
    for m in range(NBLK):
        y = jnp.concatenate([ya[m * B : (m + 1) * B], yb[m * B : (m + 1) * B]], axis=1)
        pot = along_first(y)
        for u in range(3):
            j = 3 * m + u
            part = pot[:, u * LANES : (u + 1) * LANES]
            box[pl.ds(PAD + j, B, stride=COLS), :] = part * near[pl.ds(j, B, stride=COLS), :]
            out[0, pl.ds(j, B, stride=COLS), :] = part * shifted[j * B : (j + 1) * B, :]
    for m in range(NBLK):
        js = [3 * m, 3 * m + 1, 3 * m + 2]
        for j, part in zip(js, turned(box, -e0, -e1, -e2, js)):
            out[1, pl.ds(j, B, stride=COLS), :] = part


def pair_kernel(slices, slab, round_id, ranks, tab, *refs):
    nears, refs = refs[:slices], refs[slices:]
    fars, refs = refs[:slices], refs[slices:]
    consts, refs = refs[:7], refs[7:]
    if ranks[0]:
        refs = refs[slices:]
    near_outs, refs = refs[:slices], refs[slices:]
    far_outs, refs = refs[:slices], refs[slices:]
    near, box, shifted, left_h, left_l, mid, mid2, inv_left, out = refs
    own = tab[5, 0]
    zeros = jnp.zeros((PAD, LANES), jnp.float32)
    box[:PAD, :] = zeros
    box[PAD + BOX :, :] = zeros
    for at, c in enumerate(ranks):
        slot = (round_id * slices + own) * CAP + c

        @pl.when(tab[0, slot] > 0)
        def _():
            for k in range(slices):
                start = (own ^ k) * slab
                near[pl.ds(start, slab), :] = nears[k][c]
                box[pl.ds(PAD + start, slab), :] = fars[k][c]
            one_slot(near, box, shifted, left_h, left_l, mid, mid2, inv_left, *consts, out, tab[2, slot], tab[3, slot], tab[4, slot])
            for k in range(slices):
                start = (own ^ k) * slab
                near_outs[k][c] = out[0, pl.ds(start, slab), :]
                far_outs[k][at] = out[1, pl.ds(start, slab), :]


def kept(x):
    return pltpu.with_memory_space_constraint(x, pltpu.VMEM)


def grant(mib):
    return pltpu.CompilerParams(vmem_limit_bytes=mib * 2**20)


def smem():
    return pl.BlockSpec(memory_space=pltpu.SMEM)


def vmem():
    return pl.BlockSpec(memory_space=pltpu.VMEM)


def pair_call(slices, slab, round_id, ranks, tab, nears, fars, consts, earlier):
    spots = np.arange(B * B).reshape(COLS, LANES)
    spots = jnp.asarray(np.concatenate([spots // B, spots % B]).astype(np.int32))
    operands = [tab, *map(kept, nears), *map(kept, fars), *map(kept, consts), spots, *map(kept, earlier)]
    outs = pl.pallas_call(
        functools.partial(pair_kernel, slices, slab, round_id, ranks),
        in_specs=[smem()] + [vmem()] * (len(operands) - 1),
        out_specs=[vmem()] * (2 * slices),
        out_shape=[pltpu.VMEM((CAP, slab, LANES), jnp.float32)] * slices
        + [pltpu.VMEM((len(ranks), slab, LANES), jnp.float32)] * slices,
        input_output_aliases={len(operands) - len(earlier) + k: k for k in range(len(earlier))},
        scratch_shapes=[
            pltpu.VMEM((BOX, LANES), jnp.float32),
            pltpu.VMEM((BOX + 2 * PAD, LANES), jnp.float32),
            pltpu.VMEM((BOX, LANES), jnp.float32),
            pltpu.VMEM((NBLK * B, BLK), jnp.bfloat16),
            pltpu.VMEM((NBLK * B, BLK), jnp.bfloat16),
            pltpu.VMEM((B * PITCH, LANES), jnp.float32),
            pltpu.VMEM((B * PITCH, LANES), jnp.float32),
            pltpu.VMEM((NBLK * B, ROWS_BLK * LANES), jnp.bfloat16),
            pltpu.VMEM((2, BOX, LANES), jnp.float32),
        ],
        cost_estimate=pl.CostEstimate(flops=2 * 10**9, transcendentals=0, bytes_accessed=8 * 10**6),
        compiler_params=grant(24),
    )(*operands)
    return outs[:slices], outs[slices:]


def slab_pieces(orbs, planes, o):
    if orbs == 8:
        return [(o, planes * COLS, 0)]
    tiles = orbs // 8
    high = lax.shift_right_logical(o, 3)
    return [((a * tiles + high) * COLS * 8 + (o & 7), COLS, a * COLS) for a in range(planes)]


def near_kernel(groups, slices, listed, orbs, planes, meta, values, *refs):
    rounds = groups // slices
    outs, (tab, seen) = refs[: rounds * slices], refs[rounds * slices :]
    gid = meta[0]
    own = meta[1]
    tab[5, 0] = own
    owner_at, remote_at, resident_at, count_at = 2, 2 + listed, 2 + 2 * listed, 2 + 3 * listed
    offset_at = count_at + slices
    for g in range(groups):
        seen[g] = 0
    for n in range(groups * CAP):
        tab[0, n] = 0

    def place(t, carry):
        running = 0
        home = 0
        for u in range(slices):
            running = running + meta[count_at + u]
            home = home + jnp.where(running <= t, 1, 0)
        owner = meta[owner_at + t]
        rank = seen[owner]
        seen[owner] = rank + 1
        n = (gid ^ owner) * CAP + rank
        local = home * (orbs // slices) + meta[resident_at + t]
        near_at = offset_at + 3 * (gid * orbs + local)
        far_at = offset_at + 3 * (owner * orbs + meta[remote_at + t])
        tab[0, n] = 1
        tab[1, n] = local
        for d in range(3):
            tab[2 + d, n] = meta[near_at + d] - meta[far_at + d]
        return carry

    lax.fori_loop(0, listed, place, 0)
    for q in range(rounds):
        for k in range(slices):
            for c in range(CAP):
                n = (q * slices + (own ^ k)) * CAP + c

                @pl.when(tab[0, n] > 0)
                def _():
                    for start, count, to in slab_pieces(orbs, planes, tab[1, n]):
                        outs[q * slices + k][c, to : to + count, :] = values[pl.ds(start, count, stride=8), :]


def far_kernel(groups, slices, listed, orbs, planes, lists, values, *refs):
    rounds = groups // slices
    outs, (tab, after) = refs[: rounds * slices], refs[rounds * slices :]
    gid = lists[0, 2 * listed]
    own = lists[0, 2 * listed + 1]
    after[0] = own
    for n in range(groups * CAP):
        tab[0, n] = 0

    def place(r, carry):
        def look(t, rank):
            hit = lists[gid ^ r, t] == gid

            @pl.when(hit)
            def _():
                tab[0, r * CAP + rank] = 1
                tab[1, r * CAP + rank] = lists[gid ^ r, listed + t]

            return rank + jnp.where(hit, 1, 0)

        return lax.fori_loop(0, listed, look, carry * 0)

    lax.fori_loop(0, groups, place, 0)
    for q in range(rounds):
        for k in range(slices):
            for c in range(CAP):
                n = (q * slices + (own ^ k)) * CAP + c

                @pl.when(tab[0, n] > 0)
                def _():
                    for start, count, to in slab_pieces(orbs, planes, tab[1, n]):
                        outs[q * slices + k][c, to : to + count, :] = values[pl.ds(start, count, stride=8), :]


def sum_kernel(slices, orbs, planes, near_keys, far_keys, first, near_tab, far_tab, base, *refs):
    if first:
        values, refs = refs[0], refs[1:]
    out = refs[-1]
    own = near_tab[5, 0]
    out[...] = base[...] * values[...] if first else base[...]
    for tab, keys, parts in ((near_tab, near_keys, refs), (far_tab, far_keys, refs[len(near_keys) :])):
        for part, (q, k, ranks) in zip(parts, keys):
            for at, c in enumerate(ranks):
                n = (q * slices + (own ^ k)) * CAP + c

                @pl.when(tab[0, n] > 0)
                def _():
                    for start, count, to in slab_pieces(orbs, planes, tab[1, n]):
                        rows = pl.ds(start, count, stride=8)
                        out[rows, :] = out[rows, :] - part[at, to : to + count, :]


def as_rows(x):
    orbs, planes, cells = x.shape
    x = x.transpose(1, 0, 2).reshape(planes, orbs // 8, 8, cells // LANES, LANES)
    return x.transpose(0, 1, 3, 2, 4).reshape(-1, LANES)


def operator(orbitals, local_pot, pair_owner, pair_remote, pair_resident, pair_count, offsets):
    groups = lax.axis_size("grp")
    slices = lax.axis_size("slc")
    orbs, planes, cells = orbitals.shape
    listed = pair_owner.shape[1]
    rounds = groups // slices
    slab = planes * cells // LANES
    gid = lax.axis_index("grp").astype(jnp.int32)
    sid = lax.axis_index("slc").astype(jnp.int32)
    owner = pair_owner[0, :, 0]
    meta = jnp.concatenate(
        [gid[None], sid[None], owner, pair_remote[0], pair_resident[0], pair_count[0], offsets.reshape(-1)]
    )
    line = jnp.concatenate([owner, pair_remote[0], sid[None], sid[None]])[None]
    place = lax.broadcasted_iota(jnp.int32, (groups, 2 * listed + 2), 1)
    mine = jnp.where(place == 2 * listed, lax.broadcasted_iota(jnp.int32, place.shape, 0), line)
    lists = lax.all_to_all(mine, "grp", 0, 0, tiled=True)
    rows = as_rows(orbitals)
    pot_rows = as_rows(local_pot)
    sizes = (groups, slices, listed, orbs, planes)
    keys = [(q, k) for q in range(rounds) for k in range(slices)]
    word = jax.ShapeDtypeStruct((1,), jnp.int32)
    packed = pl.pallas_call(
        functools.partial(near_kernel, *sizes),
        in_specs=[smem(), vmem()],
        out_specs=[vmem()] * len(keys) + [smem()],
        out_shape=[pltpu.VMEM((CAP, slab, LANES), jnp.float32)] * len(keys)
        + [jax.ShapeDtypeStruct((6, groups * CAP), jnp.int32)],
        scratch_shapes=[pltpu.SMEM((groups,), jnp.int32)],
        compiler_params=grant(4),
        name="near_pack",
    )(meta, rows)
    near_tab = packed[-1]
    across = [[(s, s ^ k) for s in range(slices)] for k in range(slices)]
    nears = {}
    for q, k in keys:
        nears[q, k] = packed[q * slices + k]
        if k:
            nears[q, k] = lax.ppermute(nears[q, k], "slc", across[k])
    sends = pl.pallas_call(
        functools.partial(far_kernel, *sizes),
        in_specs=[smem(), vmem()],
        out_specs=[vmem()] * len(keys) + [smem()] * 2,
        out_shape=[pltpu.VMEM((CAP, slab, LANES), jnp.float32)] * len(keys)
        + [jax.ShapeDtypeStruct((2, groups * CAP), jnp.int32), word],
        compiler_params=grant(4),
        name="far_pack",
    )(lists, rows)
    far_tab, after = sends[-2], sends[-1]

    def there(q, k):
        return [
            (g * slices + s, (g ^ (q * slices + (s ^ k))) * slices + (s ^ k))
            for g in range(groups)
            for s in range(slices)
        ]

    fars = {}
    for q, k in keys:
        fars[q, k] = lax.ppermute(sends[q * slices + k], ("grp", "slc"), there(q, k))
    consts = make_tables(after)
    every = tuple(range(CAP))
    near_back, far_back = {}, {}
    for q in range(rounds):
        earlier = []
        for ranks in rank_sets(q, rounds):
            earlier, far_out = pair_call(
                slices, slab, q, ranks, near_tab, [nears[q, k] for k in range(slices)],
                [fars[q, k] for k in range(slices)], consts, earlier
            )
            for k in range(slices):
                back = [(d, s) for s, d in there(q, k)]
                far_back[q, k, ranks] = lax.ppermute(far_out[k], ("grp", "slc"), back)
        for k in range(slices):
            near_back[q, k, every] = earlier[k] if k == 0 else lax.ppermute(earlier[k], "slc", across[k])
    last = rounds - 1
    steps = [([x for x in near_back if x[0] < last], [x for x in far_back if x[0] < last])]
    for ranks in rank_sets(last, rounds):
        steps.append(([x for x in near_back if x[0] == last and not ranks[0]], [x for x in far_back if x[::2] == (last, ranks)]))
    out = None
    for step, (near_keys, far_keys) in enumerate(steps):
        first = out is None
        ended = step == len(steps) - 1
        base = [pot_rows, rows] if first else [kept(out)]
        parts = [kept(near_back[x]) for x in near_keys] + [kept(far_back[x]) for x in far_keys]
        out = pl.pallas_call(
            functools.partial(sum_kernel, slices, orbs, planes, near_keys, far_keys, first),
            in_specs=[smem()] * 2 + [vmem()] * (len(base) + len(parts)),
            out_specs=vmem(),
            out_shape=jax.ShapeDtypeStruct(rows.shape, jnp.float32) if ended else pltpu.VMEM(rows.shape, jnp.float32),
            compiler_params=grant(6),
        )(near_tab, far_tab, *base, *parts)
    out = out.reshape(planes, orbs // 8, cells // LANES, 8, LANES).transpose(0, 1, 3, 2, 4)
    return out.reshape(planes, orbs, cells).transpose(1, 0, 2)


def rank_sets(q, rounds):
    return [(c,) for c in range(CAP)] if q == rounds - 1 else [tuple(range(CAP))]


def solution(mesh):
    in_specs = (
        P("grp", "slc", None),
        P("grp", "slc", None),
        P("grp", None, None),
        P("grp", None),
        P("grp", None),
        P("grp", None),
        P(),
    )
    return jax.shard_map(operator, mesh=mesh, in_specs=in_specs, out_specs=P("grp", "slc", None), check_vma=False)
```
